512 devices in a mesh: row: 16 (over x_lo, z), col: 32 (over y, x_hi, core).
Axes of the slice: x: 4 (x_hi: 2, x_lo: 2; x = x_hi * 2 + x_lo), y: 8, z: 8, core: 2. Of those that a mesh axis runs over, the one named last changes fastest.
Arguments:
- layer_input: bfloat16 [256, 8192], P('col', 'row'), may hold values from -6 to 6
- out_grad: bfloat16 [256, 8192], P('col', 'row'), may hold values from -6 to 6
- gate_weight: bfloat16 [8192, 28672], P('row', 'col'), may hold values from -0.0625 to 0.0625
- up_weight: bfloat16 [8192, 28672], P('row', 'col'), may hold values from -0.0625 to 0.0625
- down_weight: bfloat16 [28672, 8192], P('col', 'row'), may hold values from -0.03125 to 0.03125
Outputs:
- input_grad: bfloat16 [256, 8192], P('col', 'row')
- down_grad: bfloat16 [28672, 8192], P('col', 'row')
The draws below stay inside these ranges and needn't reach their ends.
All inputs are finite; a program needn't handle non-finite values.
Results may differ from the reference program's by a relative error of at most 0.0049.
Values may be sent and summed in bfloat16 or wider, within the bound.
A program may use at most 64 MiB of HBM per device.

```python
import jax
import jax.numpy as jnp
from jax import lax

D = 8192
FF = 28672
TOKENS = 256


def levels(rng, dims, shards, low, top_value):
    def one(axis_at, blocks):
        draws = jax.random.uniform(jax.random.fold_in(jax.random.fold_in(rng, 6), axis_at), (blocks,), jnp.float32, low / len(shards), top_value / len(shards))
        return jnp.repeat(jnp.exp(draws), dims[axis_at] // blocks).reshape((-1,) + (1,) * (len(dims) - axis_at - 1))

    loudness = one(*shards[0])
    for cut in shards[1:]:
        loudness = loudness * one(*cut)
    return loudness


def bell_draw(rng, shape, spread, reach, cuts=(), kind=jnp.bfloat16):
    values = jax.random.normal(rng, shape, jnp.float32) * spread
    if len(cuts) > 0:
        values = levels(rng, shape, cuts, -0.22, 0.18) * values
    return jnp.clip(values, min=-reach, max=reach).astype(kind)


def setup_inputs(seed: int = 0) -> dict:
    seeds = jax.random.split(jax.random.key(seed), 6)
    layer_input = bell_draw(seeds[0], (TOKENS, D), 1.0, 6.0, ((0, 32), (1, 16)))
    out_grad = bell_draw(seeds[1], (TOKENS, D), 1.0, 6.0, ((0, 32), (1, 16)))
    gate_weight = bell_draw(seeds[2], (D, FF), D ** -0.5, 0.0625, ((0, 16), (1, 32)))
    up_weight = bell_draw(seeds[3], (D, FF), D ** -0.5, 0.0625, ((0, 16), (1, 32)))
    down_weight = bell_draw(seeds[4], (FF, D), FF ** -0.5, 0.03125, ((0, 32), (1, 16)))
    return {"layer_input": layer_input, "out_grad": out_grad, "gate_weight": gate_weight, "up_weight": up_weight, "down_weight": down_weight}


def reference(layer_input, out_grad, gate_weight, up_weight, down_weight):
    gate = jnp.dot(layer_input, gate_weight, preferred_element_type=jnp.float32)
    up = jnp.dot(layer_input, up_weight, preferred_element_type=jnp.float32)
    hidden_grad = lax.dot_general(out_grad, down_weight, (((1,), (1,)), ((), ())), preferred_element_type=jnp.float32)
    sig = jax.nn.sigmoid(gate)
    silu = gate * sig
    hidden = (silu * up).astype(jnp.bfloat16)
    up_grad = (hidden_grad * silu).astype(jnp.bfloat16)
    gate_grad = (hidden_grad * up * sig * (1.0 + gate * (1.0 - sig))).astype(jnp.bfloat16)
    down_grad = lax.dot_general(hidden, out_grad, (((0,), (0,)), ((), ())), preferred_element_type=jnp.float32).astype(jnp.bfloat16)
    first = lax.dot_general(gate_grad, gate_weight, (((1,), (1,)), ((), ())), preferred_element_type=jnp.float32)
    second = lax.dot_general(up_grad, up_weight, (((1,), (1,)), ((), ())), preferred_element_type=jnp.float32)
    input_grad = (first + second).astype(jnp.bfloat16)
    return input_grad, down_grad
```

```python
import functools

import jax
import jax.numpy as jnp
from jax import lax
from jax.experimental import pallas as pl
from jax.experimental.pallas import tpu as pltpu
from jax.sharding import PartitionSpec as P

MESH = pl.DeviceIdType.MESH
WIDTHS = (256, 256, 256, 128)
OFFS = (0, 256, 512, 768)
G = len(WIDTHS)
BF16_HOPS = 2
NZ, NY, NX = 8, 8, 2
F32 = jnp.float32
BF16 = jnp.bfloat16


def contract_last(left, right):
    return lax.dot_general(
        left, right, (((1,), (1,)), ((), ())), preferred_element_type=F32
    )


def contract_first(left, right):
    return lax.dot_general(
        left, right, (((0,), (0,)), ((), ())), preferred_element_type=F32
    )


def remote(src, dst, send_sem, recv_sem, row, col):
    return pltpu.make_async_remote_copy(
        src_ref=src,
        dst_ref=dst,
        send_sem=send_sem,
        recv_sem=recv_sem,
        device_id={"row": row, "col": col},
        device_id_type=MESH,
    )


def kernel(li, og, wg_hbm, wu_hbm, wd_hbm, ig_out, dg_out, *scratch):
    scratch = list(scratch)
    take = lambda n: [scratch.pop(0) for _ in range(n)]
    (xg, wg, wu, wd) = take(4)
    part = take(G)
    sent = take(G)
    got16 = take(G)
    got32 = take(G)
    xsend = take(G)
    xrecv = take(G)
    full = take(G)
    (igs, core_got, chip_sent, chip_got) = take(4)
    (local_sem, a_send, a_recv, f_send, f_recv) = take(5)
    (rs_send, rs_recv, x_send, x_recv, ag_send, ag_recv) = take(6)
    (c_send, c_recv, d_send, d_recv) = take(4)

    row = lax.axis_index("row")
    col = lax.axis_index("col")
    z = lax.rem(row, NZ)
    x_lo = row // NZ
    core = lax.rem(col, 2)
    x_hi = lax.rem(col // 2, 2)
    y = col // 4
    s = 1 - 2 * core
    mod8 = lambda v: lax.rem(v + 16, 8)
    ahead = x_lo * NZ + mod8(z + s)
    behind = x_lo * NZ + mod8(z - s)
    across = (1 - x_lo) * NZ + z
    partner = col + s

    steps = [(dy, dx) for dy in (4, 3, 5, 2, 6, 1, 7, 0) for dx in (1, 0)][:-1]

    def chip_at(dy, dx):
        return mod8(y + dy) * 4 + lax.rem(x_hi + dx, 2) * 2

    loads = [
        pltpu.make_async_copy(
            li, xg.at[pl.ds(pl.multiple_of(col * 8, 8), 8), pl.ds(0, 512)], local_sem.at[0]
        ),
        pltpu.make_async_copy(
            og, xg.at[pl.ds(pl.multiple_of(col * 8, 8), 8), pl.ds(512, 512)], local_sem.at[1]
        ),
        pltpu.make_async_copy(wg_hbm, wg, local_sem.at[2]),
        pltpu.make_async_copy(wu_hbm, wu, local_sem.at[3]),
        pltpu.make_async_copy(wd_hbm, wd, local_sem.at[4]),
    ]
    for load in loads:
        load.start()

    barrier = pltpu.get_barrier_semaphore()
    greet = [(row, chip_at(dy, dx) + core) for dy, dx in steps]
    greet += [(row, partner), (ahead, col), (behind, col), (across, col)]
    for r, c in greet:
        pl.semaphore_signal(
            barrier, inc=1, device_id={"row": r, "col": c}, device_id_type=MESH
        )
    pl.semaphore_wait(barrier, len(greet))

    pending = []

    def go(copy):
        copy.start()
        pending.append(copy)
        return copy

    def rows_of(c):
        return xg.at[pl.ds(pl.multiple_of(c * 8, 8), 8), :]

    loads[0].wait()
    loads[1].wait()
    for i, (dy, dx) in enumerate(steps):
        go(remote(rows_of(col), rows_of(col), a_send.at[i], a_recv.at[i], row, chip_at(dy, dx) + core))
    go(remote(rows_of(col), rows_of(col), f_send.at[15], f_recv.at[15], row, partner))
    for i in reversed(range(15)):
        dy, dx = steps[i]
        src = chip_at(-dy, dx)
        remote(rows_of(src + core), rows_of(src + core), a_send.at[i], a_recv.at[i], row, col).wait_recv()
        go(remote(rows_of(src + core), rows_of(src + core), f_send.at[i], f_recv.at[i], row, partner))
    for i in reversed(range(16)):
        src = chip_at(-steps[i][0], steps[i][1]) + 1 - core if i < 15 else partner
        remote(rows_of(src), rows_of(src), f_send.at[i], f_recv.at[i], row, partner).wait_recv()
    for load in loads[2:]:
        load.wait()

    tokens = xg[:, 0:512]
    grads = xg[:, 512:1024]

    def long_copy(g, k, chunk):
        if k <= BF16_HOPS:
            src, dst = sent[g].at[0, k - 1], got16[g].at[0, k - 1]
        else:
            src, dst = part[g].at[chunk], got32[g].at[k - 3]
        return remote(src, dst, rs_send.at[g, 0, k - 1], rs_recv.at[g, 0, k - 1], ahead, col)

    def short_copy(g, k, chunk):
        if k <= BF16_HOPS:
            src, dst = sent[g].at[1, k - 1], got16[g].at[1, k - 1]
        else:
            src, dst = part[g].at[chunk], got32[g].at[2]
        return remote(src, dst, rs_send.at[g, 1, k - 1], rs_recv.at[g, 1, k - 1], behind, col)

    for g in range(G):
        w, cols = WIDTHS[g], pl.ds(OFFS[g], WIDTHS[g])
        part[g][:, 0] = jnp.dot(tokens, wg[:, cols], preferred_element_type=F32).reshape(8, 32, w)
        part[g][:, 1] = jnp.dot(tokens, wu[:, cols], preferred_element_type=F32).reshape(8, 32, w)
        part[g][:, 2] = contract_last(grads, wd[cols, :]).reshape(8, 32, w)
        far, near = mod8(z + 4 * s), mod8(z - 3 * s)
        sent[g][0, 0] = part[g][far].astype(BF16)
        go(long_copy(g, 1, far))
        sent[g][1, 0] = part[g][near].astype(BF16)
        go(short_copy(g, 1, near))
    for k in (2, 3, 4):
        for g in range(G):
            chunk = mod8(z + (5 - k) * s)
            long_copy(g, k - 1, chunk).wait_recv()
            if k - 1 <= BF16_HOPS:
                value = got16[g][0, k - 2].astype(F32) + part[g][chunk]
            else:
                value = got32[g][k - 4] + part[g][chunk]
            if k <= BF16_HOPS:
                sent[g][0, k - 1] = value.astype(BF16)
            else:
                part[g][chunk] = value
            go(long_copy(g, k, chunk))
            if k < 4:
                chunk = mod8(z - (4 - k) * s)
                short_copy(g, k - 1, chunk).wait_recv()
                value = got16[g][1, k - 2].astype(F32) + part[g][chunk]
                if k <= BF16_HOPS:
                    sent[g][1, k - 1] = value.astype(BF16)
                else:
                    part[g][chunk] = value
                go(short_copy(g, k, chunk))

    def x_copy(g):
        return remote(xsend[g], xrecv[g], x_send.at[g], x_recv.at[g], across, col)

    def gather_copy(g, flow, k, chunk):
        return remote(
            full[g].at[chunk],
            full[g].at[chunk],
            ag_send.at[g, flow, k - 1],
            ag_recv.at[g, flow, k - 1],
            (ahead, behind)[flow],
            col,
        )

    def finish(g):
        long_copy(g, 4, z).wait_recv()
        short_copy(g, 3, z).wait_recv()
        xsend[g][...] = part[g][z] + got32[g][1] + got32[g][2]
        go(x_copy(g))

    def middle(g):
        x_copy(g).wait_recv()
        gate = xsend[g][0] + xrecv[g][0]
        up = xsend[g][1] + xrecv[g][1]
        hidden_grad = xsend[g][2] + xrecv[g][2]
        sig = jax.nn.sigmoid(gate)
        silu = gate * sig
        full[g][z, 0] = (silu * up).astype(BF16)
        full[g][z, 1] = (hidden_grad * up * sig * (1.0 + gate * (1.0 - sig))).astype(BF16)
        full[g][z, 2] = (hidden_grad * silu).astype(BF16)
        go(gather_copy(g, 0, 1, z))
        go(gather_copy(g, 1, 1, z))

    LAG = 2
    for i in range(G + LAG):
        if i < G:
            finish(i)
        if i >= LAG:
            middle(i - LAG)
    for k in (2, 3, 4):
        for g in range(G):
            chunk = mod8(z - (k - 1) * s)
            gather_copy(g, 0, k - 1, chunk).wait_recv()
            go(gather_copy(g, 0, k, chunk))
            if k < 4:
                chunk = mod8(z + (k - 1) * s)
                gather_copy(g, 1, k - 1, chunk).wait_recv()
                go(gather_copy(g, 1, k, chunk))

    total = None
    for g in range(G):
        gather_copy(g, 1, 3, mod8(z + 3 * s)).wait_recv()
        gather_copy(g, 0, 4, mod8(z - 4 * s)).wait_recv()
        w, cols = WIDTHS[g], pl.ds(OFFS[g], WIDTHS[g])
        term = contract_last(full[g][:, 1].reshape(256, w), wg[:, cols])
        term += contract_last(full[g][:, 2].reshape(256, w), wu[:, cols])
        total = term if total is None else total + term
    igs[...] = total.reshape(16, 2, 8, 512)

    core_copy = go(
        remote(igs.at[:, 1 - core], core_got, c_send.at[0], c_recv.at[0], row, partner)
    )

    def weight_grad(g):
        w, cols = WIDTHS[g], pl.ds(OFFS[g], WIDTHS[g])
        dg_out[cols, :] = contract_first(full[g][:, 0].reshape(256, w), grads).astype(BF16)

    weight_grad(0)
    core_copy.wait_recv()
    both = igs[:, core] + core_got[...]
    core_got[...] = both
    chip_sent[...] = both.astype(BF16)
    for i, (dy, dx) in enumerate(steps):
        chip = chip_at(dy, dx)
        go(
            remote(
                chip_sent.at[chip // 2], chip_got.at[i], d_send.at[i], d_recv.at[i], row, chip + core
            )
        )
    for g in range(1, G):
        weight_grad(g)
    done = core_got[col // 2]
    for i in reversed(range(15)):
        remote(chip_sent.at[0], chip_got.at[i], d_send.at[i], d_recv.at[i], row, col).wait_recv()
        done += chip_got[i].astype(F32)
    ig_out[...] = done.astype(BF16)

    for copy in pending:
        copy.wait_send()


def body(layer_input, out_grad, gate_weight, up_weight, down_weight):
    dma = pltpu.SemaphoreType.DMA
    chunks = lambda lead, kind: [pltpu.VMEM((*lead, 3, 32, w), kind) for w in WIDTHS]
    scratch = [
        pltpu.VMEM((256, 1024), BF16),
        pltpu.VMEM((512, 896), BF16),
        pltpu.VMEM((512, 896), BF16),
        pltpu.VMEM((896, 512), BF16),
        *chunks((8,), F32),
        *chunks((2, BF16_HOPS), BF16),
        *chunks((2, BF16_HOPS), BF16),
        *chunks((3,), F32),
        *chunks((), F32),
        *chunks((), F32),
        *chunks((8,), BF16),
        pltpu.VMEM((16, 2, 8, 512), F32),
        pltpu.VMEM((16, 8, 512), F32),
        pltpu.VMEM((16, 8, 512), BF16),
        pltpu.VMEM((15, 8, 512), BF16),
        dma((5,)),
        dma((15,)),
        dma((15,)),
        dma((16,)),
        dma((16,)),
        dma((G, 2, 4)),
        dma((G, 2, 4)),
        dma((G,)),
        dma((G,)),
        dma((G, 2, 4)),
        dma((G, 2, 4)),
        dma((1,)),
        dma((1,)),
        dma((15,)),
        dma((15,)),
    ]
    hbm = pl.BlockSpec(memory_space=pl.ANY)
    vmem = pl.BlockSpec(memory_space=pltpu.VMEM)
    return pl.pallas_call(
        kernel,
        out_shape=(
            jax.ShapeDtypeStruct((8, 512), BF16),
            jax.ShapeDtypeStruct((896, 512), BF16),
        ),
        in_specs=[hbm] * 5,
        out_specs=(vmem, vmem),
        scratch_shapes=scratch,
        compiler_params=pltpu.CompilerParams(
            collective_id=0, has_side_effects=True, vmem_limit_bytes=60 * 1024 * 1024
        ),
        name="swiglu_back",
    )(layer_input, out_grad, gate_weight, up_weight, down_weight)


def solution(mesh):
    return jax.shard_map(
        body,
        mesh=mesh,
        in_specs=(
            P("col", "row"),
            P("col", "row"),
            P("row", "col"),
            P("row", "col"),
            P("col", "row"),
        ),
        out_specs=(P("col", "row"), P("col", "row")),
        check_vma=False,
    )
```

```python
import jax
import jax.numpy as jnp
from jax import lax
from jax.experimental import pallas as pl
from jax.experimental.pallas import tpu as pltpu
from jax.sharding import PartitionSpec as P

MESH = pl.DeviceIdType.MESH
WIDTHS = (256, 256, 256, 128)
OFFS = (0, 256, 512, 768)
G = len(WIDTHS)
NZ = 8
SIDE = (True, True, False, False)
FIRST = (True, False, False, False)
F32 = jnp.float32
BF16 = jnp.bfloat16


def contract_last(left, right):
    return lax.dot_general(
        left, right, (((1,), (1,)), ((), ())), preferred_element_type=F32
    )


def contract_first(left, right):
    return lax.dot_general(
        left, right, (((0,), (0,)), ((), ())), preferred_element_type=F32
    )


def early(g):
    return 1 if FIRST[g] else 2


def remote(src, dst, send_sem, recv_sem, row, col):
    return pltpu.make_async_remote_copy(
        src_ref=src,
        dst_ref=dst,
        send_sem=send_sem,
        recv_sem=recv_sem,
        device_id={"row": row, "col": col},
        device_id_type=MESH,
    )


def kernel(li, og, wg_hbm, wu_hbm, wd_hbm, ig_out, dg_out, *scratch):
    scratch = list(scratch)
    take = lambda n: [scratch.pop(0) for _ in range(n)]
    (xg, wg, wu, wd) = take(4)
    part = take(G)
    sent = take(G)
    got16 = take(G)
    got32 = take(G)
    xsend = take(G)
    xrecv = take(G)
    full = take(G)
    (igs, core_got, chip_sent, chip_got) = take(4)
    (local_sem, a_send, a_recv, f_send, f_recv) = take(5)
    (rs_send, rs_recv, x_send, x_recv, ag_send, ag_recv, side_send, side_recv) = take(8)
    (c_send, c_recv, d_send, d_recv) = take(4)

    row = lax.axis_index("row")
    col = lax.axis_index("col")
    z = lax.rem(row, NZ)
    x_lo = row // NZ
    core = lax.rem(col, 2)
    x_hi = lax.rem(col // 2, 2)
    y = col // 4
    s = 1 - 2 * core
    mod8 = lambda v: lax.rem(v + 16, 8)
    ahead = x_lo * NZ + mod8(z + s)
    behind = x_lo * NZ + mod8(z - s)
    across = (1 - x_lo) * NZ + z
    partner = col + s

    steps = [(dy, dx) for dy in (4, 3, 5, 2, 6, 1, 7, 0) for dx in (1, 0)][:-1]

    def chip_at(dy, dx):
        return mod8(y + dy) * 4 + lax.rem(x_hi + dx, 2) * 2

    loads = [
        pltpu.make_async_copy(
            li, xg.at[pl.ds(pl.multiple_of(col * 8, 8), 8), pl.ds(0, 512)], local_sem.at[0]
        ),
        pltpu.make_async_copy(
            og, xg.at[pl.ds(pl.multiple_of(col * 8, 8), 8), pl.ds(512, 512)], local_sem.at[1]
        ),
        pltpu.make_async_copy(wg_hbm, wg, local_sem.at[2]),
        pltpu.make_async_copy(wu_hbm, wu, local_sem.at[3]),
        pltpu.make_async_copy(wd_hbm, wd, local_sem.at[4]),
    ]
    for load in loads:
        load.start()

    barrier = pltpu.get_barrier_semaphore()
    greet = [(row, chip_at(dy, dx) + core) for dy, dx in steps]
    greet += [(row, partner), (ahead, col), (behind, col), (across, col)]
    for r, c in greet:
        pl.semaphore_signal(
            barrier, inc=1, device_id={"row": r, "col": c}, device_id_type=MESH
        )
    pl.semaphore_wait(barrier, len(greet))

    pending = []

    def go(copy):
        copy.start()
        pending.append(copy)
        return copy

    def rows_of(c):
        return xg.at[pl.ds(pl.multiple_of(c * 8, 8), 8), :]

    loads[0].wait()
    loads[1].wait()
    for i, (dy, dx) in enumerate(steps):
        go(remote(rows_of(col), rows_of(col), a_send.at[i], a_recv.at[i], row, chip_at(dy, dx) + core))
    go(remote(rows_of(col), rows_of(col), f_send.at[15], f_recv.at[15], row, partner))
    for i in reversed(range(15)):
        dy, dx = steps[i]
        src = chip_at(-dy, dx)
        remote(rows_of(src + core), rows_of(src + core), a_send.at[i], a_recv.at[i], row, col).wait_recv()
        go(remote(rows_of(src + core), rows_of(src + core), f_send.at[i], f_recv.at[i], row, partner))
    for i in reversed(range(16)):
        src = chip_at(-steps[i][0], steps[i][1]) + 1 - core if i < 15 else partner
        remote(rows_of(src), rows_of(src), f_send.at[i], f_recv.at[i], row, partner).wait_recv()
    for load in loads[2:]:
        load.wait()

    tokens = xg[:, 0:512]
    grads = xg[:, 512:1024]

    def part_ref(g, chunk):
        return part[g].at[x_lo, chunk] if FIRST[g] else part[g].at[chunk]

    def own(g, chunk):
        value = part_ref(g, chunk)[...]
        return value + xrecv[g][chunk].astype(F32) if FIRST[g] else value

    def ring_copy(g, flow, k, chunk):
        e = early(g)
        if k <= e:
            src, dst = sent[g].at[flow, k - 1], got16[g].at[flow, k - 1]
        else:
            src, dst = part_ref(g, chunk), got32[g].at[(k - e - 1) + flow * (4 - e)]
        return remote(
            src, dst, rs_send.at[g, flow, k - 1], rs_recv.at[g, flow, k - 1], (ahead, behind)[flow], col
        )

    def ring_got(g, flow, k):
        ring_copy(g, flow, k, z).wait_recv()
        e = early(g)
        if k <= e:
            return got16[g][flow, k - 1].astype(F32)
        return got32[g][(k - e - 1) + flow * (4 - e)]

    def products(g):
        w, cols = WIDTHS[g], pl.ds(OFFS[g], WIDTHS[g])
        for m in range(3):
            if m == 2:
                value = contract_last(grads, wd[cols, :])
            else:
                value = jnp.dot(tokens, (wg, wu)[m][:, cols], preferred_element_type=F32)
            if FIRST[g]:
                value = value.reshape(8, 2, 16, w)
                part[g][0, :, m] = value[:, 0]
                part[g][1, :, m] = value[:, 1]
            else:
                part[g][:, m] = value.reshape(8, 32, w)

    def ring_stage(g, k):
        for flow in (0, 1):
            if flow == 1 and k == 4:
                continue
            chunk = mod8(z + (5 - k) * s) if flow == 0 else mod8(z - (4 - k) * s)
            if k == 1:
                if FIRST[g]:
                    pair_copy(g, k - 1 + 4 * flow, chunk).wait_recv()
                value = own(g, chunk)
            else:
                if FIRST[g]:
                    pair_copy(g, k - 1 + 4 * flow, chunk).wait_recv()
                value = ring_got(g, flow, k - 1) + own(g, chunk)
            if k <= early(g):
                sent[g][flow, k - 1] = value.astype(BF16)
            elif k > 1 or FIRST[g]:
                part_ref(g, chunk)[...] = value
            go(ring_copy(g, flow, k, chunk))

    def pair_copy(g, i, chunk):
        return remote(xsend[g].at[chunk], xrecv[g].at[chunk], x_send.at[g, i], x_recv.at[g, i], across, col)

    def pair_stage(g):
        xsend[g][...] = part[g][1 - x_lo].astype(BF16)
        for i, chunk in ((0, 4), (4, -3), (1, 3), (5, -2), (2, 2), (6, -1), (3, 1), (7, 0)):
            go(pair_copy(g, i, mod8(z + chunk * s)))

    later = [g for g in range(G) if not FIRST[g]] + [g for g in range(G) if FIRST[g]]
    for g in range(G):
        products(g)
        if FIRST[g]:
            pair_stage(g)
        else:
            ring_stage(g, 1)
    for g in range(G):
        if FIRST[g]:
            ring_stage(g, 1)
    for k in (2, 3, 4):
        for g in later:
            ring_stage(g, k)

    def x_copy(g):
        src, dst = xsend[g], xrecv[g]
        if SIDE[g]:
            src, dst = src.at[1 - x_lo], dst.at[1 - x_lo]
        return remote(src, dst, x_send.at[g, 0], x_recv.at[g, 0], across, col)

    def gather_copy(g, flow, k, chunk):
        ref = full[g].at[chunk, x_lo] if SIDE[g] else full[g].at[chunk]
        return remote(ref, ref, ag_send.at[g, flow, k - 1], ag_recv.at[g, flow, k - 1], (ahead, behind)[flow], col)

    def side_copy(g, i, chunk, half):
        ref = full[g].at[chunk, half]
        return remote(ref, ref, side_send.at[g, i], side_recv.at[g, i], across, col)

    def finish(g):
        value = part[g][z] + ring_got(g, 0, 4) + ring_got(g, 1, 3)
        xsend[g][0] = value[:, 0:16]
        xsend[g][1] = value[:, 16:32]
        go(x_copy(g))

    def middle(g):
        mine = x_lo if SIDE[g] else slice(None)
        if FIRST[g]:
            pair_copy(g, 7, z).wait_recv()
            value = own(g, z) + ring_got(g, 0, 4) + ring_got(g, 1, 3)
        else:
            x_copy(g).wait_recv()
            value = xsend[g][mine] + xrecv[g][mine]
        gate, up, hidden_grad = (value[..., m, :, :] for m in range(3))
        sig = jax.nn.sigmoid(gate)
        silu = gate * sig
        full[g][z, mine, 0] = (silu * up).astype(BF16)
        full[g][z, mine, 1] = (hidden_grad * up * sig * (1.0 + gate * (1.0 - sig))).astype(BF16)
        full[g][z, mine, 2] = (hidden_grad * silu).astype(BF16)
        go(gather_copy(g, 0, 1, z))
        go(gather_copy(g, 1, 1, z))
        if SIDE[g]:
            go(side_copy(g, 0, z, x_lo))

    def forward(g, k):
        chunk = mod8(z - (k - 1) * s)
        gather_copy(g, 0, k - 1, chunk).wait_recv()
        if k < 5:
            go(gather_copy(g, 0, k, chunk))
        if SIDE[g] and k > 1:
            go(side_copy(g, k - 1, chunk, x_lo))
        if k < 5:
            chunk = mod8(z + (k - 1) * s)
            gather_copy(g, 1, k - 1, chunk).wait_recv()
            if k < 4:
                go(gather_copy(g, 1, k, chunk))
            if SIDE[g]:
                go(side_copy(g, k + 3, chunk, x_lo))

    for g in range(G):
        if not FIRST[g]:
            finish(g)
    for g in range(G):
        middle(g)
    for k in (2, 3, 4):
        for g in range(G):
            forward(g, k)
    for g in range(G):
        if SIDE[g]:
            forward(g, 5)

    def gathered(g, m):
        return full[g][:, :, m].reshape(256, WIDTHS[g])

    total = None
    for g in sorted(range(G), key=lambda g: SIDE[g]):
        if SIDE[g]:
            for i in range(8):
                chunk = mod8(z - i * s) if i < 5 else mod8(z + (i - 4) * s)
                side_copy(g, i, chunk, 1 - x_lo).wait_recv()
        else:
            forward(g, 5)
        w, cols = WIDTHS[g], pl.ds(OFFS[g], WIDTHS[g])
        term = contract_last(gathered(g, 1), wg[:, cols])
        term += contract_last(gathered(g, 2), wu[:, cols])
        total = term if total is None else total + term
    igs[...] = total.reshape(16, 2, 8, 512)

    core_copy = go(
        remote(igs.at[:, 1 - core], core_got, c_send.at[0], c_recv.at[0], row, partner)
    )

    def weight_grad(g):
        w, cols = WIDTHS[g], pl.ds(OFFS[g], WIDTHS[g])
        dg_out[cols, :] = contract_first(gathered(g, 0), grads).astype(BF16)

    weight_grad(0)
    core_copy.wait_recv()
    both = igs[:, core] + core_got[...]
    core_got[...] = both
    chip_sent[...] = both.astype(BF16)
    for i, (dy, dx) in enumerate(steps):
        chip = chip_at(dy, dx)
        go(
            remote(
                chip_sent.at[chip // 2], chip_got.at[i], d_send.at[i], d_recv.at[i], row, chip + core
            )
        )
    for g in range(1, G):
        weight_grad(g)
    done = core_got[col // 2]
    for i in reversed(range(15)):
        remote(chip_sent.at[0], chip_got.at[i], d_send.at[i], d_recv.at[i], row, col).wait_recv()
        done += chip_got[i].astype(F32)
    ig_out[...] = done.astype(BF16)

    for copy in pending:
        copy.wait_send()


def body(layer_input, out_grad, gate_weight, up_weight, down_weight):
    dma = pltpu.SemaphoreType.DMA

    def rings(late, first, late_kind, first_kind):
        return [
            pltpu.VMEM((*first, 3, 16, w), first_kind) if f else pltpu.VMEM((*late, 3, 32, w), late_kind)
            for w, f in zip(WIDTHS, FIRST)
        ]

    def halves(first_kind, late_kind):
        return [
            pltpu.VMEM((8, 3, 16, w), first_kind) if f else pltpu.VMEM((2, 3, 16, w), late_kind)
            for w, f in zip(WIDTHS, FIRST)
        ]

    scratch = [
        pltpu.VMEM((256, 1024), BF16),
        pltpu.VMEM((512, 896), BF16),
        pltpu.VMEM((512, 896), BF16),
        pltpu.VMEM((896, 512), BF16),
        *rings((8,), (2, 8), F32, F32),
        *rings((2, 2), (2, 1), BF16, BF16),
        *rings((2, 2), (2, 1), BF16, BF16),
        *rings((3,), (5,), F32, F32),
        *halves(BF16, F32),
        *halves(BF16, F32),
        *[pltpu.VMEM((8, 2, 3, 16, w), BF16) for w in WIDTHS],
        pltpu.VMEM((16, 2, 8, 512), F32),
        pltpu.VMEM((16, 8, 512), F32),
        pltpu.VMEM((16, 8, 512), BF16),
        pltpu.VMEM((15, 8, 512), BF16),
        dma((5,)),
        dma((15,)),
        dma((15,)),
        dma((16,)),
        dma((16,)),
        dma((G, 2, 4)),
        dma((G, 2, 4)),
        dma((G, 8)),
        dma((G, 8)),
        dma((G, 2, 4)),
        dma((G, 2, 4)),
        dma((G, 8)),
        dma((G, 8)),
        dma((1,)),
        dma((1,)),
        dma((15,)),
        dma((15,)),
    ]
    hbm = pl.BlockSpec(memory_space=pl.ANY)
    vmem = pl.BlockSpec(memory_space=pltpu.VMEM)
    return pl.pallas_call(
        kernel,
        out_shape=(
            jax.ShapeDtypeStruct((8, 512), BF16),
            jax.ShapeDtypeStruct((896, 512), BF16),
        ),
        in_specs=[hbm] * 5,
        out_specs=(vmem, vmem),
        scratch_shapes=scratch,
        compiler_params=pltpu.CompilerParams(
            collective_id=0, has_side_effects=True, vmem_limit_bytes=53 * 1024 * 1024
        ),
        name="swiglu_back",
    )(layer_input, out_grad, gate_weight, up_weight, down_weight)


def solution(mesh):
    return jax.shard_map(
        body,
        mesh=mesh,
        in_specs=(
            P("col", "row"),
            P("col", "row"),
            P("row", "col"),
            P("row", "col"),
            P("col", "row"),
        ),
        out_specs=(P("col", "row"), P("col", "row")),
        check_vma=False,
    )
```

```python
import jax
import jax.numpy as jnp
from jax import lax
from jax.experimental import pallas as pl
from jax.experimental.pallas import tpu as pltpu
from jax.sharding import PartitionSpec as P

MESH = pl.DeviceIdType.MESH
WIDTHS = (256, 256, 256, 128)
OFFS = (0, 256, 512, 768)
G = len(WIDTHS)
NZ = 8
SIDE = (True, True, False, False)
FIRST = (True, False, False, False)
F32 = jnp.float32
BF16 = jnp.bfloat16


def contract_last(left, right):
    return lax.dot_general(
        left, right, (((1,), (1,)), ((), ())), preferred_element_type=F32
    )


def contract_first(left, right):
    return lax.dot_general(
        left, right, (((0,), (0,)), ((), ())), preferred_element_type=F32
    )


def early(g):
    return 1 if FIRST[g] else 2


def remote(src, dst, send_sem, recv_sem, row, col):
    return pltpu.make_async_remote_copy(
        src_ref=src,
        dst_ref=dst,
        send_sem=send_sem,
        recv_sem=recv_sem,
        device_id={"row": row, "col": col},
        device_id_type=MESH,
    )


def kernel(li, og, wg_hbm, wu_hbm, wd_hbm, ig_out, dg_out, *scratch):
    scratch = list(scratch)
    take = lambda n: [scratch.pop(0) for _ in range(n)]
    (xg, wg, wu, wd) = take(4)
    part = take(G)
    sent = take(G)
    got16 = take(G)
    got32 = take(G)
    xsend = take(G)
    xrecv = take(G)
    full = take(G)
    (igs, core_got, chip_sent, chip_got) = take(4)
    (local_sem, a_send, a_recv, f_send, f_recv) = take(5)
    (rs_send, rs_recv, x_send, x_recv, ag_send, ag_recv, side_send, side_recv) = take(8)
    (c_send, c_recv, d_send, d_recv) = take(4)

    row = lax.axis_index("row")
    col = lax.axis_index("col")
    z = lax.rem(row, NZ)
    x_lo = row // NZ
    core = lax.rem(col, 2)
    x_hi = lax.rem(col // 2, 2)
    y = col // 4
    s = 1 - 2 * core
    mod8 = lambda v: lax.rem(v + 16, 8)
    ahead = x_lo * NZ + mod8(z + s)
    behind = x_lo * NZ + mod8(z - s)
    across = (1 - x_lo) * NZ + z
    partner = col + s

    steps = [(dy, dx) for dy in (4, 3, 5, 2, 6, 1, 7, 0) for dx in (1, 0)][:-1]

    def chip_at(dy, dx):
        return mod8(y + dy) * 4 + lax.rem(x_hi + dx, 2) * 2

    loads = [
        pltpu.make_async_copy(
            li, xg.at[pl.ds(pl.multiple_of(col * 8, 8), 8), pl.ds(0, 512)], local_sem.at[0]
        ),
        pltpu.make_async_copy(
            og, xg.at[pl.ds(pl.multiple_of(col * 8, 8), 8), pl.ds(512, 512)], local_sem.at[1]
        ),
        pltpu.make_async_copy(wg_hbm, wg, local_sem.at[2]),
        pltpu.make_async_copy(wu_hbm, wu, local_sem.at[3]),
        pltpu.make_async_copy(wd_hbm, wd, local_sem.at[4]),
    ]
    for load in loads:
        load.start()

    barrier = pltpu.get_barrier_semaphore()
    greet = [(row, chip_at(dy, dx) + core) for dy, dx in steps]
    greet += [(row, partner), (ahead, col), (behind, col), (across, col)]
    for r, c in greet:
        pl.semaphore_signal(
            barrier, inc=1, device_id={"row": r, "col": c}, device_id_type=MESH
        )
    pl.semaphore_wait(barrier, len(greet))

    pending = []

    def go(copy):
        copy.start()
        pending.append(copy)
        return copy

    def rows_of(c):
        return xg.at[pl.ds(pl.multiple_of(c * 8, 8), 8), :]

    loads[0].wait()
    loads[1].wait()
    for i, (dy, dx) in enumerate(steps):
        go(remote(rows_of(col), rows_of(col), a_send.at[i], a_recv.at[i], row, chip_at(dy, dx) + core))
    go(remote(rows_of(col), rows_of(col), f_send.at[15], f_recv.at[15], row, partner))
    for i in reversed(range(15)):
        dy, dx = steps[i]
        src = chip_at(-dy, dx)
        remote(rows_of(src + core), rows_of(src + core), a_send.at[i], a_recv.at[i], row, col).wait_recv()
        go(remote(rows_of(src + core), rows_of(src + core), f_send.at[i], f_recv.at[i], row, partner))
    for i in reversed(range(16)):
        src = chip_at(-steps[i][0], steps[i][1]) + 1 - core if i < 15 else partner
        remote(rows_of(src), rows_of(src), f_send.at[i], f_recv.at[i], row, partner).wait_recv()
    for load in loads[2:]:
        load.wait()

    tokens = xg[:, 0:512]
    grads = xg[:, 512:1024]

    def part_ref(g, chunk):
        return part[g].at[x_lo, chunk] if FIRST[g] else part[g].at[chunk]

    def own(g, chunk):
        value = part_ref(g, chunk)[...]
        return value + xrecv[g][chunk].astype(F32) if FIRST[g] else value

    def ring_copy(g, flow, k, chunk):
        e = early(g)
        if k <= e:
            src, dst = sent[g].at[flow, k - 1], got16[g].at[flow, k - 1]
        else:
            src, dst = part_ref(g, chunk), got32[g].at[(k - e - 1) + flow * (4 - e)]
        return remote(
            src, dst, rs_send.at[g, flow, k - 1], rs_recv.at[g, flow, k - 1], (ahead, behind)[flow], col
        )

    def ring_got(g, flow, k):
        ring_copy(g, flow, k, z).wait_recv()
        e = early(g)
        if k <= e:
            return got16[g][flow, k - 1].astype(F32)
        return got32[g][(k - e - 1) + flow * (4 - e)]

    def products(g):
        w, cols = WIDTHS[g], pl.ds(OFFS[g], WIDTHS[g])
        for m in range(3):
            if m == 2:
                value = contract_last(grads, wd[cols, :])
            else:
                value = jnp.dot(tokens, (wg, wu)[m][:, cols], preferred_element_type=F32)
            if FIRST[g]:
                value = value.reshape(8, 2, 16, w)
                part[g][0, :, m] = value[:, 0]
                part[g][1, :, m] = value[:, 1]
            else:
                part[g][:, m] = value.reshape(8, 32, w)

    def ring_stage(g, k):
        for flow in (0, 1):
            if flow == 1 and k == 4:
                continue
            chunk = mod8(z + (5 - k) * s) if flow == 0 else mod8(z - (4 - k) * s)
            if k == 1:
                if FIRST[g]:
                    pair_copy(g, k - 1 + 4 * flow, chunk).wait_recv()
                value = own(g, chunk)
            else:
                if FIRST[g]:
                    pair_copy(g, k - 1 + 4 * flow, chunk).wait_recv()
                value = ring_got(g, flow, k - 1) + own(g, chunk)
            if k <= early(g):
                sent[g][flow, k - 1] = value.astype(BF16)
            elif k > 1 or FIRST[g]:
                part_ref(g, chunk)[...] = value
            go(ring_copy(g, flow, k, chunk))

    def pair_copy(g, i, chunk):
        return remote(xsend[g].at[chunk], xrecv[g].at[chunk], x_send.at[g, i], x_recv.at[g, i], across, col)

    def pair_stage(g):
        xsend[g][...] = part[g][1 - x_lo].astype(BF16)
        for i, chunk in ((0, 4), (4, -3), (1, 3), (5, -2), (2, 2), (6, -1), (3, 1), (7, 0)):
            go(pair_copy(g, i, mod8(z + chunk * s)))

    later = [g for g in range(G) if not FIRST[g]] + [g for g in range(G) if FIRST[g]]
    for g in range(G):
        products(g)
        if FIRST[g]:
            pair_stage(g)
        else:
            ring_stage(g, 1)
    for g in range(G):
        if FIRST[g]:
            ring_stage(g, 1)
    for k in (2, 3, 4):
        for g in later:
            ring_stage(g, k)

    def x_copy(g):
        src, dst = xsend[g], xrecv[g]
        if SIDE[g]:
            src, dst = src.at[1 - x_lo], dst.at[1 - x_lo]
        return remote(src, dst, x_send.at[g, 0], x_recv.at[g, 0], across, col)

    def gather_copy(g, flow, k, chunk):
        ref = full[g].at[chunk, x_lo] if SIDE[g] else full[g].at[chunk]
        return remote(ref, ref, ag_send.at[g, flow, k - 1], ag_recv.at[g, flow, k - 1], (ahead, behind)[flow], col)

    def side_copy(g, i, chunk, half):
        ref = full[g].at[chunk, half]
        return remote(ref, ref, side_send.at[g, i], side_recv.at[g, i], across, col)

    def finish(g):
        value = part[g][z] + ring_got(g, 0, 4) + ring_got(g, 1, 3)
        xsend[g][0] = value[:, 0:16]
        xsend[g][1] = value[:, 16:32]
        go(x_copy(g))

    def middle(g):
        mine = x_lo if SIDE[g] else slice(None)
        if FIRST[g]:
            pair_copy(g, 7, z).wait_recv()
            value = own(g, z) + ring_got(g, 0, 4) + ring_got(g, 1, 3)
        else:
            x_copy(g).wait_recv()
            value = xsend[g][mine] + xrecv[g][mine]
        gate, up, hidden_grad = (value[..., m, :, :] for m in range(3))
        sig = jax.nn.sigmoid(gate)
        silu = gate * sig
        full[g][z, mine, 0] = (silu * up).astype(BF16)
        full[g][z, mine, 1] = (hidden_grad * up * sig * (1.0 + gate * (1.0 - sig))).astype(BF16)
        full[g][z, mine, 2] = (hidden_grad * silu).astype(BF16)
        go(gather_copy(g, 0, 1, z))
        go(gather_copy(g, 1, 1, z))
        if SIDE[g]:
            go(side_copy(g, 0, z, x_lo))

    def forward(g, k):
        chunk = mod8(z - (k - 1) * s)
        gather_copy(g, 0, k - 1, chunk).wait_recv()
        if k < 5:
            go(gather_copy(g, 0, k, chunk))
        if SIDE[g] and k > 1:
            go(side_copy(g, k - 1, chunk, x_lo))
        if k < 5:
            chunk = mod8(z + (k - 1) * s)
            gather_copy(g, 1, k - 1, chunk).wait_recv()
            if k < 4:
                go(gather_copy(g, 1, k, chunk))
            if SIDE[g]:
                go(side_copy(g, k + 3, chunk, x_lo))

    for g in range(G):
        if not FIRST[g]:
            finish(g)
    for g in range(G):
        middle(g)
    def gathered(g, m):
        return full[g][:, :, m].reshape(256, WIDTHS[g])

    def chunk_at(d):
        return mod8(z - d * s)

    def core_copy(chunk):
        return remote(
            igs.at[chunk, :, 1 - core], core_got.at[chunk], c_send.at[chunk], c_recv.at[chunk], row, partner
        )

    def input_grad(distances):
        total = None
        for g in sorted(range(G), key=lambda g: SIDE[g]):
            w, cols = WIDTHS[g], pl.ds(OFFS[g], WIDTHS[g])
            if SIDE[g]:
                for d in distances:
                    side_copy(g, d if d >= 0 else 4 - d, chunk_at(d), 1 - x_lo).wait_recv()
            for m, weight in ((1, wg), (2, wu)):
                left = [full[g][chunk_at(d), :, m].reshape(32, w) for d in distances]
                term = contract_last(jnp.concatenate(left, axis=0), weight[:, cols])
                total = term if total is None else total + term
        for n, d in enumerate(distances):
            igs[chunk_at(d)] = total[32 * n : 32 * n + 32].reshape(2, 2, 8, 512)
        for d in distances:
            go(core_copy(chunk_at(d)))

    def to_owners(distances):
        for d in distances:
            chunk = chunk_at(d)
            core_copy(chunk).wait_recv()
            both = igs[chunk, :, core] + core_got[chunk]
            core_got[chunk] = both
            chip_sent[chunk] = both.astype(BF16)
            for half in (0, 1):
                i = mod8(chunk - y) * 2 + lax.rem(half + x_hi, 2)

                @pl.when(i != 0)
                def _():
                    remote(
                        chip_sent.at[chunk, half],
                        chip_got.at[i],
                        d_send.at[i],
                        d_recv.at[i],
                        row,
                        chunk * 4 + half * 2 + core,
                    ).start()

    def weight_grad(g):
        w, cols = WIDTHS[g], pl.ds(OFFS[g], WIDTHS[g])
        dg_out[cols, :] = contract_first(gathered(g, 0), grads).astype(BF16)

    for k in (2, 3):
        for g in range(G):
            forward(g, k)
    input_grad((0, 1, -1))
    for g in range(G):
        forward(g, 4)
    input_grad((2, -2))
    to_owners((0, 1, -1))
    for g in range(G):
        forward(g, 5)
    to_owners((2, -2))
    input_grad((3, -3, 4))
    weight_grad(0)
    to_owners((3, -3, 4))
    for g in range(1, G):
        weight_grad(g)
    done = core_got[y, x_hi]
    for i in range(15, 0, -1):
        owner_copy = remote(chip_sent.at[0, 0], chip_got.at[i], d_send.at[i], d_recv.at[i], row, partner)
        owner_copy.wait_recv()
        done += chip_got[i].astype(F32)
        pending.append(owner_copy)
    ig_out[...] = done.astype(BF16)

    for copy in pending:
        copy.wait_send()


def body(layer_input, out_grad, gate_weight, up_weight, down_weight):
    dma = pltpu.SemaphoreType.DMA

    def rings(late, first, late_kind, first_kind):
        return [
            pltpu.VMEM((*first, 3, 16, w), first_kind) if f else pltpu.VMEM((*late, 3, 32, w), late_kind)
            for w, f in zip(WIDTHS, FIRST)
        ]

    def halves(first_kind, late_kind):
        return [
            pltpu.VMEM((8, 3, 16, w), first_kind) if f else pltpu.VMEM((2, 3, 16, w), late_kind)
            for w, f in zip(WIDTHS, FIRST)
        ]

    scratch = [
        pltpu.VMEM((256, 1024), BF16),
        pltpu.VMEM((512, 896), BF16),
        pltpu.VMEM((512, 896), BF16),
        pltpu.VMEM((896, 512), BF16),
        *rings((8,), (2, 8), F32, F32),
        *rings((2, 2), (2, 1), BF16, BF16),
        *rings((2, 2), (2, 1), BF16, BF16),
        *rings((3,), (5,), F32, F32),
        *halves(BF16, F32),
        *halves(BF16, F32),
        *[pltpu.VMEM((8, 2, 3, 16, w), BF16) for w in WIDTHS],
        pltpu.VMEM((8, 2, 2, 8, 512), F32),
        pltpu.VMEM((8, 2, 8, 512), F32),
        pltpu.VMEM((8, 2, 8, 512), BF16),
        pltpu.VMEM((16, 8, 512), BF16),
        dma((5,)),
        dma((15,)),
        dma((15,)),
        dma((16,)),
        dma((16,)),
        dma((G, 2, 4)),
        dma((G, 2, 4)),
        dma((G, 8)),
        dma((G, 8)),
        dma((G, 2, 4)),
        dma((G, 2, 4)),
        dma((G, 8)),
        dma((G, 8)),
        dma((8,)),
        dma((8,)),
        dma((16,)),
        dma((16,)),
    ]
    hbm = pl.BlockSpec(memory_space=pltpu.HBM)
    vmem = pl.BlockSpec(memory_space=pltpu.VMEM)
    layer_input = pltpu.with_memory_space_constraint(layer_input, pltpu.HBM)
    out_grad = pltpu.with_memory_space_constraint(out_grad, pltpu.HBM)
    return pl.pallas_call(
        kernel,
        out_shape=(
            jax.ShapeDtypeStruct((8, 512), BF16),
            jax.ShapeDtypeStruct((896, 512), BF16),
        ),
        in_specs=[hbm] * 5,
        out_specs=(vmem, vmem),
        scratch_shapes=scratch,
        compiler_params=pltpu.CompilerParams(
            collective_id=0, has_side_effects=True, vmem_limit_bytes=53 * 1024 * 1024
        ),
        name="swiglu_back",
    )(layer_input, out_grad, gate_weight, up_weight, down_weight)


def solution(mesh):
    return jax.shard_map(
        body,
        mesh=mesh,
        in_specs=(
            P("col", "row"),
            P("col", "row"),
            P("row", "col"),
            P("row", "col"),
            P("col", "row"),
        ),
        out_specs=(P("col", "row"), P("col", "row")),
        check_vma=False,
    )
```

```python
import jax
import jax.numpy as jnp
from jax import lax
from jax.experimental import pallas as pl
from jax.experimental.pallas import tpu as pltpu
from jax.sharding import PartitionSpec as P

MESH = pl.DeviceIdType.MESH
WIDTHS = (256, 256, 256, 128)
OFFS = (0, 256, 512, 768)
G = len(WIDTHS)
NZ = 8
SIDE = (True, True, False, False)
FIRST = (True, False, False, False)
F32 = jnp.float32
BF16 = jnp.bfloat16


def contract_last(left, right):
    return lax.dot_general(
        left, right, (((1,), (1,)), ((), ())), preferred_element_type=F32
    )


def contract_first(left, right):
    return lax.dot_general(
        left, right, (((0,), (0,)), ((), ())), preferred_element_type=F32
    )


def early(g):
    return 1 if FIRST[g] else 2


def remote(src, dst, send_sem, recv_sem, row, col):
    return pltpu.make_async_remote_copy(
        src_ref=src,
        dst_ref=dst,
        send_sem=send_sem,
        recv_sem=recv_sem,
        device_id={"row": row, "col": col},
        device_id_type=MESH,
    )


def kernel(li, og, wg_hbm, wu_hbm, wd_hbm, ig_out, dg_out, *scratch):
    scratch = list(scratch)
    take = lambda n: [scratch.pop(0) for _ in range(n)]
    (xg, wg, wu, wd) = take(4)
    part = take(G)
    sent = take(G)
    got16 = take(G)
    got32 = take(G)
    xsend = take(G)
    xrecv = take(G)
    full = take(G)
    (igs, core_got, chip_sent, chip_got) = take(4)
    (local_sem, a_send, a_recv, q_send, q_recv, f_send, f_recv) = take(7)
    (rs_send, rs_recv, x_send, x_recv, ag_send, ag_recv, side_send, side_recv) = take(8)
    (c_send, c_recv, d_send, d_recv) = take(4)

    row = lax.axis_index("row")
    col = lax.axis_index("col")
    z = lax.rem(row, NZ)
    x_lo = row // NZ
    core = lax.rem(col, 2)
    x_hi = lax.rem(col // 2, 2)
    y = col // 4
    s = 1 - 2 * core
    mod8 = lambda v: lax.rem(v + 16, 8)
    ahead = x_lo * NZ + mod8(z + s)
    behind = x_lo * NZ + mod8(z - s)
    across = (1 - x_lo) * NZ + z
    partner = col + s

    def chip_at(dy, dx):
        return mod8(y + dy) * 4 + lax.rem(x_hi + dx, 2) * 2

    loads = [
        pltpu.make_async_copy(
            li, xg.at[pl.ds(pl.multiple_of(col * 8, 8), 8), pl.ds(0, 512)], local_sem.at[0]
        ),
        pltpu.make_async_copy(
            og, xg.at[pl.ds(pl.multiple_of(col * 8, 8), 8), pl.ds(512, 512)], local_sem.at[1]
        ),
        pltpu.make_async_copy(wg_hbm, wg, local_sem.at[2]),
        pltpu.make_async_copy(wu_hbm, wu, local_sem.at[3]),
        pltpu.make_async_copy(wd_hbm, wd, local_sem.at[4]),
    ]
    for load in loads:
        load.start()

    barrier = pltpu.get_barrier_semaphore()
    greet = [(row, chip_at(dy, 0) + core) for dy in (2, -2, 1, -1)]
    greet += [(row, chip_at(0, 1) + core), (row, partner), (ahead, col), (behind, col), (across, col)]
    for r, c in greet:
        pl.semaphore_signal(
            barrier, inc=1, device_id={"row": r, "col": c}, device_id_type=MESH
        )
    pl.semaphore_wait(barrier, len(greet))

    pending = []

    def go(copy):
        copy.start()
        pending.append(copy)
        return copy

    def rows_of(c):
        return xg.at[pl.ds(pl.multiple_of(c * 8, 8), 8), :]

    pair = chip_at(0, 1) + core

    def y_copy(source, to):
        c = chip_at(source, 0) + core
        ahead_y = chip_at(source + to, 0) + core
        return remote(rows_of(c), rows_of(c), a_send.at[to % 8], a_recv.at[to % 8], row, ahead_y)

    def q_copy(dy, c):
        return remote(rows_of(c), rows_of(c), q_send.at[dy % 8], q_recv.at[dy % 8], row, pair)

    def f_copy(dx, dy, c):
        return remote(rows_of(c), rows_of(c), f_send.at[dx, dy % 8], f_recv.at[dx, dy % 8], row, partner)

    loads[0].wait()
    loads[1].wait()
    for to in (2, -2, 1, -1):
        go(y_copy(0, to))
    go(q_copy(0, col))
    go(f_copy(0, 0, col))
    def products(g, sources):
        w, cols = WIDTHS[g], pl.ds(OFFS[g], WIDTHS[g])
        chunks = [mod8(y + dy) for dy in sources]

        def rows(columns):
            blocks = [xg[pl.ds(pl.multiple_of(32 * c, 32), 32), columns] for c in chunks]
            return jnp.concatenate(blocks, axis=0)

        for m in range(3):
            if m == 2:
                value = contract_last(rows(slice(512, 1024)), wd[cols, :])
            else:
                value = jnp.dot(rows(slice(0, 512)), (wg, wu)[m][:, cols], preferred_element_type=F32)
            for n, c in enumerate(chunks):
                if FIRST[g]:
                    part[g][0, c, m] = value[32 * n : 32 * n + 16]
                    part[g][1, c, m] = value[32 * n + 16 : 32 * n + 32]
                else:
                    part[g][c, m] = value[32 * n : 32 * n + 32]

    def y_arrives(to):
        c = chip_at(-to, 0) + core
        y_copy(-to, to).wait_recv()
        if to == 2:
            go(y_copy(-2, 4))
            go(y_copy(-2, 3))
        if to == -2:
            go(y_copy(2, -3))
        go(q_copy(to, c))
        go(f_copy(0, to, c))

    def q_arrives(to):
        c = chip_at(-to, 1) + core
        q_copy(to, c).wait_recv()
        go(f_copy(1, to, c))

    def f_arrive(to):
        for dx in (0, 1):
            f_copy(dx, to, chip_at(-to, dx) + 1 - core).wait_recv()

    near, far = (0, 1, -1, 2, -2), (3, -3, 4)
    for to in near[1:]:
        y_arrives(to)
    for to in near:
        q_arrives(to)
    for to in far:
        y_arrives(to)
    for load in loads[2:]:
        load.wait()
    for to in near:
        f_arrive(to)
    for g in range(G):
        products(g, near)
    for to in far:
        q_arrives(to)
    for to in far:
        f_arrive(to)
    grads = xg[:, 512:1024]

    def part_ref(g, chunk):
        return part[g].at[x_lo, chunk] if FIRST[g] else part[g].at[chunk]

    def own(g, chunk):
        value = part_ref(g, chunk)[...]
        return value + xrecv[g][chunk].astype(F32) if FIRST[g] else value

    def ring_copy(g, flow, k, chunk):
        e = early(g)
        if k <= e:
            src, dst = sent[g].at[flow, k - 1], got16[g].at[flow, k - 1]
        else:
            src, dst = part_ref(g, chunk), got32[g].at[(k - e - 1) + flow * (4 - e)]
        return remote(
            src, dst, rs_send.at[g, flow, k - 1], rs_recv.at[g, flow, k - 1], (ahead, behind)[flow], col
        )

    def ring_got(g, flow, k):
        ring_copy(g, flow, k, z).wait_recv()
        e = early(g)
        if k <= e:
            return got16[g][flow, k - 1].astype(F32)
        return got32[g][(k - e - 1) + flow * (4 - e)]

    def ring_stage(g, k):
        for flow in (0, 1):
            if flow == 1 and k == 4:
                continue
            chunk = mod8(z + (5 - k) * s) if flow == 0 else mod8(z - (4 - k) * s)
            if k == 1:
                if FIRST[g]:
                    pair_copy(g, k - 1 + 4 * flow, chunk).wait_recv()
                value = own(g, chunk)
            else:
                if FIRST[g]:
                    pair_copy(g, k - 1 + 4 * flow, chunk).wait_recv()
                value = ring_got(g, flow, k - 1) + own(g, chunk)
            if k <= early(g):
                sent[g][flow, k - 1] = value.astype(BF16)
            elif k > 1 or FIRST[g]:
                part_ref(g, chunk)[...] = value
            go(ring_copy(g, flow, k, chunk))

    def pair_copy(g, i, chunk):
        return remote(xsend[g].at[chunk], xrecv[g].at[chunk], x_send.at[g, i], x_recv.at[g, i], across, col)

    def pair_stage(g):
        xsend[g][...] = part[g][1 - x_lo].astype(BF16)
        for i, chunk in ((0, 4), (4, -3), (1, 3), (5, -2), (2, 2), (6, -1), (3, 1), (7, 0)):
            go(pair_copy(g, i, mod8(z + chunk * s)))

    later = [g for g in range(G) if not FIRST[g]] + [g for g in range(G) if FIRST[g]]
    for g in range(G):
        products(g, far)
        if FIRST[g]:
            pair_stage(g)
        else:
            ring_stage(g, 1)
    for g in range(G):
        if FIRST[g]:
            ring_stage(g, 1)
    for k in (2, 3, 4):
        for g in later:
            ring_stage(g, k)

    def x_copy(g):
        src, dst = xsend[g], xrecv[g]
        if SIDE[g]:
            src, dst = src.at[1 - x_lo], dst.at[1 - x_lo]
        return remote(src, dst, x_send.at[g, 0], x_recv.at[g, 0], across, col)

    def gather_copy(g, flow, k, chunk):
        ref = full[g].at[chunk, x_lo] if SIDE[g] else full[g].at[chunk]
        return remote(ref, ref, ag_send.at[g, flow, k - 1], ag_recv.at[g, flow, k - 1], (ahead, behind)[flow], col)

    def side_copy(g, i, chunk, half):
        ref = full[g].at[chunk, half]
        return remote(ref, ref, side_send.at[g, i], side_recv.at[g, i], across, col)

    def finish(g):
        value = part[g][z] + ring_got(g, 0, 4) + ring_got(g, 1, 3)
        xsend[g][0] = value[:, 0:16]
        xsend[g][1] = value[:, 16:32]
        go(x_copy(g))

    def middle(g):
        mine = x_lo if SIDE[g] else slice(None)
        if FIRST[g]:
            pair_copy(g, 7, z).wait_recv()
            value = own(g, z) + ring_got(g, 0, 4) + ring_got(g, 1, 3)
        else:
            x_copy(g).wait_recv()
            value = xsend[g][mine] + xrecv[g][mine]
        gate, up, hidden_grad = (value[..., m, :, :] for m in range(3))
        sig = jax.nn.sigmoid(gate)
        silu = gate * sig
        full[g][z, mine, 0] = (silu * up).astype(BF16)
        full[g][z, mine, 1] = (hidden_grad * up * sig * (1.0 + gate * (1.0 - sig))).astype(BF16)
        full[g][z, mine, 2] = (hidden_grad * silu).astype(BF16)
        go(gather_copy(g, 0, 1, z))
        go(gather_copy(g, 1, 1, z))
        if SIDE[g]:
            go(side_copy(g, 0, z, x_lo))

    def forward(g, k):
        chunk = mod8(z - (k - 1) * s)
        gather_copy(g, 0, k - 1, chunk).wait_recv()
        if k < 5:
            go(gather_copy(g, 0, k, chunk))
        if SIDE[g] and k > 1:
            go(side_copy(g, k - 1, chunk, x_lo))
        if k < 5:
            chunk = mod8(z + (k - 1) * s)
            gather_copy(g, 1, k - 1, chunk).wait_recv()
            if k < 4:
                go(gather_copy(g, 1, k, chunk))
            if SIDE[g]:
                go(side_copy(g, k + 3, chunk, x_lo))

    for g in range(G):
        if not FIRST[g]:
            finish(g)
    for g in range(G):
        middle(g)
    def gathered(g, m):
        return full[g][:, :, m].reshape(256, WIDTHS[g])

    def chunk_at(d):
        return mod8(z - d * s)

    def core_copy(chunk):
        return remote(
            igs.at[chunk, :, 1 - core], core_got.at[chunk], c_send.at[chunk], c_recv.at[chunk], row, partner
        )

    def input_grad(distances):
        total = None
        for g in sorted(range(G), key=lambda g: SIDE[g]):
            w, cols = WIDTHS[g], pl.ds(OFFS[g], WIDTHS[g])
            if SIDE[g]:
                for d in distances:
                    side_copy(g, d if d >= 0 else 4 - d, chunk_at(d), 1 - x_lo).wait_recv()
            for m, weight in ((1, wg), (2, wu)):
                left = [full[g][chunk_at(d), :, m].reshape(32, w) for d in distances]
                term = contract_last(jnp.concatenate(left, axis=0), weight[:, cols])
                total = term if total is None else total + term
        for n, d in enumerate(distances):
            igs[chunk_at(d)] = total[32 * n : 32 * n + 32].reshape(2, 2, 8, 512)
        for d in distances:
            go(core_copy(chunk_at(d)))

    def to_owners(distances):
        for d in distances:
            chunk = chunk_at(d)
            core_copy(chunk).wait_recv()
            both = igs[chunk, :, core] + core_got[chunk]
            core_got[chunk] = both
            chip_sent[chunk] = both.astype(BF16)
            for half in (0, 1):
                i = mod8(chunk - y) * 2 + lax.rem(half + x_hi, 2)

                @pl.when(i != 0)
                def _():
                    remote(
                        chip_sent.at[chunk, half],
                        chip_got.at[i],
                        d_send.at[i],
                        d_recv.at[i],
                        row,
                        chunk * 4 + half * 2 + core,
                    ).start()

    def weight_grad(g):
        w, cols = WIDTHS[g], pl.ds(OFFS[g], WIDTHS[g])
        dg_out[cols, :] = contract_first(gathered(g, 0), grads).astype(BF16)

    for k in (2, 3):
        for g in range(G):
            forward(g, k)
    input_grad((0, 1, -1))
    for g in range(G):
        forward(g, 4)
    input_grad((2, -2))
    to_owners((0, 1, -1))
    for g in range(G):
        forward(g, 5)
    to_owners((2, -2))
    input_grad((3, -3, 4))
    weight_grad(0)
    to_owners((3, -3, 4))
    for g in range(1, G):
        weight_grad(g)
    done = core_got[y, x_hi]
    for i in range(15, 0, -1):
        owner_copy = remote(chip_sent.at[0, 0], chip_got.at[i], d_send.at[i], d_recv.at[i], row, partner)
        owner_copy.wait_recv()
        done += chip_got[i].astype(F32)
        pending.append(owner_copy)
    ig_out[...] = done.astype(BF16)

    for copy in pending:
        copy.wait_send()


def body(layer_input, out_grad, gate_weight, up_weight, down_weight):
    dma = pltpu.SemaphoreType.DMA

    def rings(late, first, late_kind, first_kind):
        return [
            pltpu.VMEM((*first, 3, 16, w), first_kind) if f else pltpu.VMEM((*late, 3, 32, w), late_kind)
            for w, f in zip(WIDTHS, FIRST)
        ]

    def halves(first_kind, late_kind):
        return [
            pltpu.VMEM((8, 3, 16, w), first_kind) if f else pltpu.VMEM((2, 3, 16, w), late_kind)
            for w, f in zip(WIDTHS, FIRST)
        ]

    scratch = [
        pltpu.VMEM((256, 1024), BF16),
        pltpu.VMEM((512, 896), BF16),
        pltpu.VMEM((512, 896), BF16),
        pltpu.VMEM((896, 512), BF16),
        *rings((8,), (2, 8), F32, F32),
        *rings((2, 2), (2, 1), BF16, BF16),
        *rings((2, 2), (2, 1), BF16, BF16),
        *rings((3,), (5,), F32, F32),
        *halves(BF16, F32),
        *halves(BF16, F32),
        *[pltpu.VMEM((8, 2, 3, 16, w), BF16) for w in WIDTHS],
        pltpu.VMEM((8, 2, 2, 8, 512), F32),
        pltpu.VMEM((8, 2, 8, 512), F32),
        pltpu.VMEM((8, 2, 8, 512), BF16),
        pltpu.VMEM((16, 8, 512), BF16),
        dma((5,)),
        dma((8,)),
        dma((8,)),
        dma((8,)),
        dma((8,)),
        dma((2, 8)),
        dma((2, 8)),
        dma((G, 2, 4)),
        dma((G, 2, 4)),
        dma((G, 8)),
        dma((G, 8)),
        dma((G, 2, 4)),
        dma((G, 2, 4)),
        dma((G, 8)),
        dma((G, 8)),
        dma((8,)),
        dma((8,)),
        dma((16,)),
        dma((16,)),
    ]
    hbm = pl.BlockSpec(memory_space=pltpu.HBM)
    vmem = pl.BlockSpec(memory_space=pltpu.VMEM)
    layer_input = pltpu.with_memory_space_constraint(layer_input, pltpu.HBM)
    out_grad = pltpu.with_memory_space_constraint(out_grad, pltpu.HBM)
    return pl.pallas_call(
        kernel,
        out_shape=(
            jax.ShapeDtypeStruct((8, 512), BF16),
            jax.ShapeDtypeStruct((896, 512), BF16),
        ),
        in_specs=[hbm] * 5,
        out_specs=(vmem, vmem),
        scratch_shapes=scratch,
        compiler_params=pltpu.CompilerParams(
            collective_id=0, has_side_effects=True, vmem_limit_bytes=53 * 1024 * 1024
        ),
        name="swiglu_back",
    )(layer_input, out_grad, gate_weight, up_weight, down_weight)


def solution(mesh):
    return jax.shard_map(
        body,
        mesh=mesh,
        in_specs=(
            P("col", "row"),
            P("col", "row"),
            P("row", "col"),
            P("row", "col"),
            P("col", "row"),
        ),
        out_specs=(P("col", "row"), P("col", "row")),
        check_vma=False,
    )
```

```python
import jax
import jax.numpy as jnp
from jax import lax
from jax.experimental import pallas as pl
from jax.experimental.pallas import tpu as pltpu
from jax.sharding import PartitionSpec as P

MESH = pl.DeviceIdType.MESH
WIDTHS = (256, 256, 256, 128)
OFFS = (0, 256, 512, 768)
G = len(WIDTHS)
NZ = 8
SIDE = (True, True, True, False)
FIRST = (True, False, False, False)
F32 = jnp.float32
BF16 = jnp.bfloat16


def contract_last(left, right):
    return lax.dot_general(
        left, right, (((1,), (1,)), ((), ())), preferred_element_type=F32
    )


def contract_first(left, right):
    return lax.dot_general(
        left, right, (((0,), (0,)), ((), ())), preferred_element_type=F32
    )


def early(g):
    return 1 if FIRST[g] else 2


def remote(src, dst, send_sem, recv_sem, row, col):
    return pltpu.make_async_remote_copy(
        src_ref=src,
        dst_ref=dst,
        send_sem=send_sem,
        recv_sem=recv_sem,
        device_id={"row": row, "col": col},
        device_id_type=MESH,
    )


def kernel(li, og, wg_hbm, wu_hbm, wd_hbm, ig_out, dg_out, *scratch):
    scratch = list(scratch)
    take = lambda n: [scratch.pop(0) for _ in range(n)]
    (xg, wg, wu, wd) = take(4)
    part = take(G)
    sent = take(G)
    got16 = take(G)
    got32 = take(G)
    xsend = take(G)
    xrecv = take(G)
    full = take(G)
    (igs, core_got, chip_sent, chip_got) = take(4)
    (local_sem, a_send, a_recv, q_send, q_recv, f_send, f_recv) = take(7)
    (rs_send, rs_recv, x_send, x_recv, ag_send, ag_recv, side_send, side_recv) = take(8)
    (c_send, c_recv, d_send, d_recv) = take(4)

    row = lax.axis_index("row")
    col = lax.axis_index("col")
    z = lax.rem(row, NZ)
    x_lo = row // NZ
    core = lax.rem(col, 2)
    x_hi = lax.rem(col // 2, 2)
    y = col // 4
    s = 1 - 2 * core
    mod8 = lambda v: lax.rem(v + 16, 8)
    ahead = x_lo * NZ + mod8(z + s)
    behind = x_lo * NZ + mod8(z - s)
    across = (1 - x_lo) * NZ + z
    partner = col + s

    def chip_at(dy, dx):
        return mod8(y + dy) * 4 + lax.rem(x_hi + dx, 2) * 2

    loads = [
        pltpu.make_async_copy(
            li, xg.at[pl.ds(pl.multiple_of(col * 8, 8), 8), pl.ds(0, 512)], local_sem.at[0]
        ),
        pltpu.make_async_copy(
            og, xg.at[pl.ds(pl.multiple_of(col * 8, 8), 8), pl.ds(512, 512)], local_sem.at[1]
        ),
        pltpu.make_async_copy(wg_hbm, wg, local_sem.at[2]),
        pltpu.make_async_copy(wu_hbm, wu, local_sem.at[3]),
        pltpu.make_async_copy(wd_hbm, wd, local_sem.at[4]),
    ]
    for load in loads:
        load.start()

    barrier = pltpu.get_barrier_semaphore()
    greet = [(row, chip_at(dy, 0) + core) for dy in (2, -2, 1, -1)]
    greet += [(row, chip_at(0, 1) + core), (row, partner), (ahead, col), (behind, col), (across, col)]
    for r, c in greet:
        pl.semaphore_signal(
            barrier, inc=1, device_id={"row": r, "col": c}, device_id_type=MESH
        )
    pl.semaphore_wait(barrier, len(greet))

    pending = []

    def go(copy):
        copy.start()
        pending.append(copy)
        return copy

    def rows_of(c):
        return xg.at[pl.ds(pl.multiple_of(c * 8, 8), 8), :]

    pair = chip_at(0, 1) + core

    def y_copy(source, to):
        c = chip_at(source, 0) + core
        ahead_y = chip_at(source + to, 0) + core
        return remote(rows_of(c), rows_of(c), a_send.at[to % 8], a_recv.at[to % 8], row, ahead_y)

    def q_copy(dy, c):
        return remote(rows_of(c), rows_of(c), q_send.at[dy % 8], q_recv.at[dy % 8], row, pair)

    def f_copy(dx, dy, c):
        return remote(rows_of(c), rows_of(c), f_send.at[dx, dy % 8], f_recv.at[dx, dy % 8], row, partner)

    loads[0].wait()
    loads[1].wait()
    for to in (2, -2, 1, -1):
        go(y_copy(0, to))
    go(q_copy(0, col))
    go(f_copy(0, 0, col))
    def products(g, sources):
        w, cols = WIDTHS[g], pl.ds(OFFS[g], WIDTHS[g])
        chunks = [mod8(y + dy) for dy in sources]

        def rows(columns):
            blocks = [xg[pl.ds(pl.multiple_of(32 * c, 32), 32), columns] for c in chunks]
            return jnp.concatenate(blocks, axis=0)

        for m in range(3):
            if m == 2:
                value = contract_last(rows(slice(512, 1024)), wd[cols, :])
            else:
                value = jnp.dot(rows(slice(0, 512)), (wg, wu)[m][:, cols], preferred_element_type=F32)
            for n, c in enumerate(chunks):
                if FIRST[g]:
                    part[g][0, c, m] = value[32 * n : 32 * n + 16]
                    part[g][1, c, m] = value[32 * n + 16 : 32 * n + 32]
                else:
                    part[g][c, m] = value[32 * n : 32 * n + 32]

    def y_arrives(to):
        c = chip_at(-to, 0) + core
        y_copy(-to, to).wait_recv()
        if to == 2:
            go(y_copy(-2, 4))
            go(y_copy(-2, 3))
        if to == -2:
            go(y_copy(2, -3))
        go(q_copy(to, c))
        go(f_copy(0, to, c))

    def q_arrives(to):
        c = chip_at(-to, 1) + core
        q_copy(to, c).wait_recv()
        go(f_copy(1, to, c))

    def f_arrive(to):
        for dx in (0, 1):
            f_copy(dx, to, chip_at(-to, dx) + 1 - core).wait_recv()

    near, far = (0, 1, -1, 2, -2), (3, -3, 4)
    for to in near[1:]:
        y_arrives(to)
    q_arrives(0)
    for to in (1, -1):
        q_arrives(to)
    for to in far:
        y_arrives(to)
    for to in (2, -2):
        q_arrives(to)
    for load in loads[2:]:
        load.wait()
    for to in near:
        f_arrive(to)
    for g in range(G):
        products(g, near)
    for to in far:
        q_arrives(to)
    for to in far:
        f_arrive(to)
    grads = xg[:, 512:1024]

    def part_ref(g, chunk):
        return part[g].at[x_lo, chunk] if FIRST[g] else part[g].at[chunk]

    def own(g, chunk):
        value = part_ref(g, chunk)[...]
        return value + xrecv[g][chunk].astype(F32) if FIRST[g] else value

    def ring_copy(g, flow, k, chunk):
        e = early(g)
        if k <= e:
            src, dst = sent[g].at[flow, k - 1], got16[g].at[flow, k - 1]
        else:
            src, dst = part_ref(g, chunk), got32[g].at[(k - e - 1) + flow * (4 - e)]
        return remote(
            src, dst, rs_send.at[g, flow, k - 1], rs_recv.at[g, flow, k - 1], (ahead, behind)[flow], col
        )

    def ring_got(g, flow, k):
        ring_copy(g, flow, k, z).wait_recv()
        e = early(g)
        if k <= e:
            return got16[g][flow, k - 1].astype(F32)
        return got32[g][(k - e - 1) + flow * (4 - e)]

    def ring_stage(g, k):
        for flow in (0, 1):
            if flow == 1 and k == 4:
                continue
            chunk = mod8(z + (5 - k) * s) if flow == 0 else mod8(z - (4 - k) * s)
            if k == 1:
                if FIRST[g]:
                    pair_copy(g, k - 1 + 4 * flow, chunk).wait_recv()
                value = own(g, chunk)
            else:
                if FIRST[g]:
                    pair_copy(g, k - 1 + 4 * flow, chunk).wait_recv()
                value = ring_got(g, flow, k - 1) + own(g, chunk)
            if k <= early(g):
                sent[g][flow, k - 1] = value.astype(BF16)
            elif k > 1 or FIRST[g]:
                part_ref(g, chunk)[...] = value
            go(ring_copy(g, flow, k, chunk))

    def pair_copy(g, i, chunk):
        return remote(xsend[g].at[chunk], xrecv[g].at[chunk], x_send.at[g, i], x_recv.at[g, i], across, col)

    def pair_stage(g):
        xsend[g][...] = part[g][1 - x_lo].astype(BF16)
        for i, chunk in ((0, 4), (4, -3), (1, 3), (5, -2), (2, 2), (6, -1), (3, 1), (7, 0)):
            go(pair_copy(g, i, mod8(z + chunk * s)))

    later = [g for g in range(G) if not FIRST[g]] + [g for g in range(G) if FIRST[g]]
    for g in range(G):
        products(g, far)
        if FIRST[g]:
            pair_stage(g)
        else:
            ring_stage(g, 1)
    for g in range(G):
        if FIRST[g]:
            ring_stage(g, 1)
    for k in (2, 3, 4):
        for g in later:
            ring_stage(g, k)

    def x_copy(g):
        src, dst = xsend[g], xrecv[g]
        if SIDE[g]:
            src, dst = src.at[1 - x_lo], dst.at[1 - x_lo]
        return remote(src, dst, x_send.at[g, 0], x_recv.at[g, 0], across, col)

    def gather_copy(g, flow, k, chunk):
        ref = full[g].at[chunk, x_lo] if SIDE[g] else full[g].at[chunk]
        return remote(ref, ref, ag_send.at[g, flow, k - 1], ag_recv.at[g, flow, k - 1], (ahead, behind)[flow], col)

    def side_copy(g, i, chunk, half):
        ref = full[g].at[chunk, half]
        return remote(ref, ref, side_send.at[g, i], side_recv.at[g, i], across, col)

    def finish(g):
        value = part[g][z] + ring_got(g, 0, 4) + ring_got(g, 1, 3)
        xsend[g][0] = value[:, 0:16]
        xsend[g][1] = value[:, 16:32]
        go(x_copy(g))

    def middle(g):
        mine = x_lo if SIDE[g] else slice(None)
        if FIRST[g]:
            pair_copy(g, 7, z).wait_recv()
            value = own(g, z) + ring_got(g, 0, 4) + ring_got(g, 1, 3)
        else:
            x_copy(g).wait_recv()
            value = xsend[g][mine] + xrecv[g][mine]
        gate, up, hidden_grad = (value[..., m, :, :] for m in range(3))
        sig = jax.nn.sigmoid(gate)
        silu = gate * sig
        full[g][z, mine, 0] = (silu * up).astype(BF16)
        full[g][z, mine, 1] = (hidden_grad * up * sig * (1.0 + gate * (1.0 - sig))).astype(BF16)
        full[g][z, mine, 2] = (hidden_grad * silu).astype(BF16)
        go(gather_copy(g, 0, 1, z))
        go(gather_copy(g, 1, 1, z))
        if SIDE[g]:
            go(side_copy(g, 0, z, x_lo))

    def forward(g, k):
        chunk = mod8(z - (k - 1) * s)
        gather_copy(g, 0, k - 1, chunk).wait_recv()
        if k < 5:
            go(gather_copy(g, 0, k, chunk))
        if SIDE[g] and k > 1:
            go(side_copy(g, k - 1, chunk, x_lo))
        if k < 5:
            chunk = mod8(z + (k - 1) * s)
            gather_copy(g, 1, k - 1, chunk).wait_recv()
            if k < 4:
                go(gather_copy(g, 1, k, chunk))
            if SIDE[g]:
                go(side_copy(g, k + 3, chunk, x_lo))

    for g in range(G):
        if not FIRST[g]:
            finish(g)
    for g in range(G):
        middle(g)
    def gathered(g, m):
        return full[g][:, :, m].reshape(256, WIDTHS[g])

    def chunk_at(d):
        return mod8(z - d * s)

    def core_copy(chunk):
        return remote(
            igs.at[chunk, :, 1 - core], core_got.at[chunk], c_send.at[chunk], c_recv.at[chunk], row, partner
        )

    def input_grad(distances):
        total = None
        for g in sorted(range(G), key=lambda g: SIDE[g]):
            w, cols = WIDTHS[g], pl.ds(OFFS[g], WIDTHS[g])
            if SIDE[g]:
                for d in distances:
                    side_copy(g, d if d >= 0 else 4 - d, chunk_at(d), 1 - x_lo).wait_recv()
            for m, weight in ((1, wg), (2, wu)):
                left = [full[g][chunk_at(d), :, m].reshape(32, w) for d in distances]
                term = contract_last(jnp.concatenate(left, axis=0), weight[:, cols])
                total = term if total is None else total + term
        for n, d in enumerate(distances):
            igs[chunk_at(d)] = total[32 * n : 32 * n + 32].reshape(2, 2, 8, 512)
        for d in distances:
            go(core_copy(chunk_at(d)))

    def to_owners(distances):
        for d in distances:
            chunk = chunk_at(d)
            core_copy(chunk).wait_recv()
            both = igs[chunk, :, core] + core_got[chunk]
            core_got[chunk] = both
            chip_sent[chunk] = both.astype(BF16)
            for half in (0, 1):
                i = mod8(chunk - y) * 2 + lax.rem(half + x_hi, 2)

                @pl.when(i != 0)
                def _():
                    remote(
                        chip_sent.at[chunk, half],
                        chip_got.at[i],
                        d_send.at[i],
                        d_recv.at[i],
                        row,
                        chunk * 4 + half * 2 + core,
                    ).start()

    def weight_grad(g):
        w, cols = WIDTHS[g], pl.ds(OFFS[g], WIDTHS[g])
        dg_out[cols, :] = contract_first(gathered(g, 0), grads).astype(BF16)

    for k in (2, 3):
        for g in range(G):
            forward(g, k)
    input_grad((0, 1, -1))
    for g in range(G):
        forward(g, 4)
    input_grad((2, -2))
    to_owners((0, 1, -1))
    for g in range(G):
        forward(g, 5)
    to_owners((2, -2))
    input_grad((3, -3, 4))
    weight_grad(0)
    to_owners((3, -3, 4))
    for g in range(1, G):
        weight_grad(g)
    done = core_got[y, x_hi]
    for i in range(15, 0, -1):
        owner_copy = remote(chip_sent.at[0, 0], chip_got.at[i], d_send.at[i], d_recv.at[i], row, partner)
        owner_copy.wait_recv()
        done += chip_got[i].astype(F32)
        pending.append(owner_copy)
    ig_out[...] = done.astype(BF16)

    for copy in pending:
        copy.wait_send()


def body(layer_input, out_grad, gate_weight, up_weight, down_weight):
    dma = pltpu.SemaphoreType.DMA

    def rings(late, first, late_kind, first_kind):
        return [
            pltpu.VMEM((*first, 3, 16, w), first_kind) if f else pltpu.VMEM((*late, 3, 32, w), late_kind)
            for w, f in zip(WIDTHS, FIRST)
        ]

    def halves(first_kind, late_kind):
        return [
            pltpu.VMEM((8, 3, 16, w), first_kind) if f else pltpu.VMEM((2, 3, 16, w), late_kind)
            for w, f in zip(WIDTHS, FIRST)
        ]

    scratch = [
        pltpu.VMEM((256, 1024), BF16),
        pltpu.VMEM((512, 896), BF16),
        pltpu.VMEM((512, 896), BF16),
        pltpu.VMEM((896, 512), BF16),
        *rings((8,), (2, 8), F32, F32),
        *rings((2, 2), (2, 1), BF16, BF16),
        *rings((2, 2), (2, 1), BF16, BF16),
        *rings((3,), (5,), F32, F32),
        *halves(BF16, F32),
        *halves(BF16, F32),
        *[pltpu.VMEM((8, 2, 3, 16, w), BF16) for w in WIDTHS],
        pltpu.VMEM((8, 2, 2, 8, 512), F32),
        pltpu.VMEM((8, 2, 8, 512), F32),
        pltpu.VMEM((8, 2, 8, 512), BF16),
        pltpu.VMEM((16, 8, 512), BF16),
        dma((5,)),
        dma((8,)),
        dma((8,)),
        dma((8,)),
        dma((8,)),
        dma((2, 8)),
        dma((2, 8)),
        dma((G, 2, 4)),
        dma((G, 2, 4)),
        dma((G, 8)),
        dma((G, 8)),
        dma((G, 2, 4)),
        dma((G, 2, 4)),
        dma((G, 8)),
        dma((G, 8)),
        dma((8,)),
        dma((8,)),
        dma((16,)),
        dma((16,)),
    ]
    hbm = pl.BlockSpec(memory_space=pltpu.HBM)
    vmem = pl.BlockSpec(memory_space=pltpu.VMEM)
    layer_input = pltpu.with_memory_space_constraint(layer_input, pltpu.HBM)
    out_grad = pltpu.with_memory_space_constraint(out_grad, pltpu.HBM)
    return pl.pallas_call(
        kernel,
        out_shape=(
            jax.ShapeDtypeStruct((8, 512), BF16),
            jax.ShapeDtypeStruct((896, 512), BF16),
        ),
        in_specs=[hbm] * 5,
        out_specs=(vmem, vmem),
        scratch_shapes=scratch,
        compiler_params=pltpu.CompilerParams(
            collective_id=0, has_side_effects=True, vmem_limit_bytes=53 * 1024 * 1024
        ),
        name="swiglu_back",
    )(layer_input, out_grad, gate_weight, up_weight, down_weight)


def solution(mesh):
    return jax.shard_map(
        body,
        mesh=mesh,
        in_specs=(
            P("col", "row"),
            P("col", "row"),
            P("row", "col"),
            P("row", "col"),
            P("col", "row"),
        ),
        out_specs=(P("col", "row"), P("col", "row")),
        check_vma=False,
    )
```
